128 devices in a mesh: expert: 4 (over y_lo, core), shard: 32 (over z, y_hi, x).
Axes of the slice: x: 4, y: 4 (y_hi: 2, y_lo: 2; y = y_hi * 2 + y_lo), z: 4, core: 2. Of those that a mesh axis runs over, the one named last changes fastest.
Arguments:
- master_gate: float32 [128, 2048, 768], P('expert', 'shard'), may hold values from -0.125 to 0.125
- second_gate: bfloat16 [128, 2048, 768], P('expert', 'shard'), may hold values from -0.0625 to 0.0625
- master_up: float32 [128, 2048, 768], P('expert', 'shard'), may hold values from -0.125 to 0.125
- second_up: bfloat16 [128, 2048, 768], P('expert', 'shard'), may hold values from -0.0625 to 0.0625
- router_weight: float32 [2048, 128], P('shard', 'expert'), may hold values from -0.125 to 0.125
- router_gain: float32 [2048], P('shard'), may hold values from 0.25 to 1.75
Outputs:
- final_gate: bfloat16 [128, 768, 2048], P('expert', 'shard')
- final_up: bfloat16 [128, 768, 2048], P('expert', 'shard')
- serve_router: bfloat16 [2048, 128], replicated
The draws below stay inside these ranges and needn't reach their ends.
All inputs are finite; a program needn't handle non-finite values.
Results may differ from the reference program's by a relative error of at most 0.001.
Values may be sent and summed in bfloat16 or wider, within the bound.
No kernel may reach another device: no remote copies, remote signals or barrier semaphores. Data moves between devices by JAX's collectives and lax.ppermute only.
A program may use at most 128 MiB of HBM per device.

```python
import jax
import jax.numpy as jnp

EXPERTS = 128
D_MODEL = 2048
D_EXPERT = 768


def block_levels(own_key, shape, split, low, largest):
    factor_of = 1.0
    for position, parts in split:
        steps = jax.random.uniform(jax.random.fold_in(jax.random.fold_in(own_key, 6), position), (parts,), jnp.float32, low / len(split), largest / len(split))
        factor_of = factor_of * jnp.repeat(jnp.exp(steps), shape[position] // parts).reshape((-1,) + (1,) * (len(shape) - 1 - position))
    return factor_of


def scatter_about(stream_key, dims, width, bound, shards=(), dtype=jnp.bfloat16):
    entries = jax.random.normal(stream_key, dims, jnp.float32) * width
    if len(shards) > 0:
        entries = block_levels(stream_key, dims, shards, -0.22, 0.18) * entries
    return jnp.clip(entries, min=-bound, max=bound).astype(dtype)


def setup_inputs(seed: int = 0) -> dict:
    keys = jax.random.split(jax.random.key(seed), 7)
    master_gate = scatter_about(keys[0], (EXPERTS, D_MODEL, D_EXPERT), D_MODEL ** -0.5, 0.125, ((0, 4), (1, 32)), jnp.float32)
    second_gate = scatter_about(keys[1], (EXPERTS, D_MODEL, D_EXPERT), (D_MODEL * 4) ** -0.5, 0.0625, ((0, 4), (1, 32)))
    master_up = scatter_about(keys[2], (EXPERTS, D_MODEL, D_EXPERT), D_MODEL ** -0.5, 0.125, ((0, 4), (1, 32)), jnp.float32)
    second_up = scatter_about(keys[3], (EXPERTS, D_MODEL, D_EXPERT), (D_MODEL * 4) ** -0.5, 0.0625, ((0, 4), (1, 32)))
    router_weight = scatter_about(keys[4], (D_MODEL, EXPERTS), D_MODEL ** -0.5, 0.125, ((0, 32), (1, 4)), jnp.float32)
    router_gain = jnp.clip(1.0 + 0.15 * jax.random.normal(keys[5], (D_MODEL,), jnp.float32), 0.25, 1.75)
    return {"master_gate": master_gate, "second_gate": second_gate, "master_up": master_up, "second_up": second_up, "router_weight": router_weight, "router_gain": router_gain}


def reference(master_gate, second_gate, master_up, second_up, router_weight, router_gain):
    merged_gate = master_gate + second_gate.astype(jnp.float32)
    merged_up = master_up + second_up.astype(jnp.float32)
    final_gate = merged_gate.astype(jnp.bfloat16)
    final_gate = jnp.transpose(final_gate, (0, 2, 1))
    final_up = merged_up.astype(jnp.bfloat16)
    final_up = jnp.transpose(final_up, (0, 2, 1))
    serve_router = (router_weight * router_gain[:, None]).astype(jnp.bfloat16)
    return final_gate, final_up, serve_router
```

```python
import functools

import jax
import jax.numpy as jnp
from jax import lax
from jax.experimental import pallas as pl
from jax.experimental.pallas import tpu as pltpu
from jax.sharding import PartitionSpec as P

MIB = 1 << 20
IN_STEP = 2
OUT_STEP = 4


def joined(low, high):
    half = low.shape[-1] // 2
    return (
        jnp.concatenate([low[:, :half], high[:, :half]], axis=1),
        jnp.concatenate([low[:, half:], high[:, half:]], axis=1),
    )


def pack_kernel(part, master_gate, second_gate, master_up, second_up, weight, gain, send):
    experts, rows, width = master_gate.shape
    peers = width // part
    router = (weight[...] * gain[...]).astype(jnp.bfloat16)
    half = router.shape[0] // 2
    router = jnp.concatenate([router[:half], router[half:]], axis=1)
    for peer in range(peers):
        send[peer, experts * part :, :] = router

    def body(gate, gate_change, up, up_change):
        step = pl.program_id(0)
        for pair in range(IN_STEP // 2):
            for at, (master, second) in enumerate(((gate, gate_change), (up, up_change))):
                two = slice(2 * pair, 2 * pair + 2)
                merged = master[two] + second[two].astype(jnp.float32)
                turned = merged.reshape(2 * rows, width).T.astype(jnp.bfloat16)
                first = pl.multiple_of(step * (IN_STEP * part), 2 * part) + (2 * pair + at) * part
                for peer in range(peers):
                    send[peer, pl.ds(first, part), :] = turned[peer * part : (peer + 1) * part]

    block = pl.BlockSpec((IN_STEP, rows, width), lambda i: (i, 0, 0), pipeline_mode=pl.Buffered(4))
    pltpu.emit_pipeline(body, grid=(experts // IN_STEP,), in_specs=[block] * 4)(master_gate, second_gate, master_up, second_up)


def pack(master_gate, second_gate, master_up, second_up, weight, gain, peers):
    experts, rows, width = master_gate.shape
    part = width // peers
    lines = experts * part + weight.shape[0] // 2
    big = [pltpu.with_memory_space_constraint(x, pltpu.HBM) for x in (master_gate, second_gate, master_up, second_up)]
    in_hbm = pl.BlockSpec(memory_space=pltpu.HBM)
    in_vmem = pl.BlockSpec(memory_space=pltpu.VMEM)
    return pl.pallas_call(
        functools.partial(pack_kernel, part),
        in_specs=[in_hbm] * 4 + [in_vmem] * 2,
        out_specs=in_vmem,
        out_shape=pltpu.VMEM((peers, lines, 2 * rows), jnp.bfloat16),
        compiler_params=pltpu.CompilerParams(vmem_limit_bytes=32 * MIB),
        cost_estimate=pl.CostEstimate(flops=2 * master_gate.size, bytes_accessed=12 * master_gate.size, transcendentals=0),
        name="pack",
    )(*big, weight, gain)


def unpack_kernel(part, rows, taken, final_gate, final_up):
    peers = taken.shape[0]
    step = pl.program_id(0)
    for pair in range(OUT_STEP // 2):
        for at, final in enumerate((final_gate, final_up)):
            first = pl.multiple_of(step * (OUT_STEP * part), 2 * part) + (2 * pair + at) * part
            for couple in range(peers // 2):
                lanes = slice(2 * couple * rows, (2 * couple + 2) * rows)
                final[2 * pair, :, lanes], final[2 * pair + 1, :, lanes] = joined(
                    taken[2 * couple, pl.ds(first, part), :], taken[2 * couple + 1, pl.ds(first, part), :]
                )


def unpack(taken, experts, rows, part):
    peers = taken.shape[0]
    out = jax.ShapeDtypeStruct((experts, part, peers * rows), jnp.bfloat16)
    return pl.pallas_call(
        functools.partial(unpack_kernel, part, rows),
        grid=(experts // OUT_STEP,),
        in_specs=[pl.BlockSpec(memory_space=pltpu.VMEM)],
        out_specs=[pl.BlockSpec((OUT_STEP, part, peers * rows), lambda i: (i, 0, 0))] * 2,
        out_shape=[out, out],
        compiler_params=pltpu.CompilerParams(vmem_limit_bytes=32 * MIB),
        cost_estimate=pl.CostEstimate(flops=taken.size * 64, bytes_accessed=4 * taken.size, transcendentals=0),
        name="unpack",
    )(pltpu.with_memory_space_constraint(taken, pltpu.VMEM))


def router_kernel(*refs):
    *pieces, out, turned = refs
    me = lax.axis_index("expert")
    for other, piece in enumerate(pieces):
        peers, half, lanes = piece.shape
        first = pl.multiple_of((me ^ other) * (2 * half), 2 * half)
        for couple in range(peers // 2):
            columns = slice(couple * lanes, (couple + 1) * lanes)
            turned[pl.ds(first, half), columns], turned[pl.ds(first + half, half), columns] = joined(
                piece[2 * couple], piece[2 * couple + 1]
            )
    out[...] = turned[...].T


def spread_router(own):
    columns = lax.axis_size("expert")
    pieces = [own]
    for other in range(1, columns):
        pieces.append(lax.ppermute(own, "expert", [(i, i ^ other) for i in range(columns)]))
    peers, half, lanes = own.shape
    rows = peers * lanes // 2
    return pl.pallas_call(
        router_kernel,
        in_specs=[pl.BlockSpec(memory_space=pltpu.VMEM)] * columns,
        out_specs=pl.BlockSpec(memory_space=pltpu.VMEM),
        out_shape=jax.ShapeDtypeStruct((rows, columns * 2 * half), jnp.bfloat16),
        scratch_shapes=[pltpu.VMEM((columns * 2 * half, rows), jnp.bfloat16)],
        compiler_params=pltpu.CompilerParams(vmem_limit_bytes=16 * MIB),
        name="router",
    )(*pieces)


def per_device(master_gate, second_gate, master_up, second_up, router_weight, router_gain):
    experts, rows, width = master_gate.shape
    peers = lax.axis_size("shard")
    part = width // peers
    send = pack(master_gate, second_gate, master_up, second_up, router_weight.T, router_gain[None], peers)
    taken = lax.all_to_all(send, "shard", 0, 0, tiled=True)
    serve_router = spread_router(taken[:, experts * part :])
    final_gate, final_up = unpack(taken, experts, rows, part)
    return (final_gate, final_up, serve_router)


def solution(mesh):
    placed = (
        P("expert", "shard", None),
        P("expert", "shard", None),
        P("expert", "shard", None),
        P("expert", "shard", None),
        P("shard", "expert"),
        P("shard"),
    )
    return jax.shard_map(
        per_device,
        mesh=mesh,
        in_specs=placed,
        out_specs=(P("expert", "shard", None), P("expert", "shard", None), P()),
        check_vma=False,
    )
```

```python
import functools

import jax
import jax.numpy as jnp
from jax import lax
from jax.experimental import pallas as pl
from jax.experimental.pallas import tpu as pltpu
from jax.sharding import PartitionSpec as P

MIB = 1 << 20
IN_STEP = 2
OUT_STEP = 8


def joined(low, high):
    half = low.shape[-1] // 2
    return (
        jnp.concatenate([low[:, :half], high[:, :half]], axis=1),
        jnp.concatenate([low[:, half:], high[:, half:]], axis=1),
    )


def pack_kernel(part, master_gate, second_gate, master_up, second_up, far_weight, far_gain, send, weight, gain, come):
    experts, rows, width = master_gate.shape
    peers = width // part
    fetches = (
        pltpu.make_async_copy(far_weight, weight, come.at[0]),
        pltpu.make_async_copy(far_gain, gain, come.at[1]),
    )
    for fetch in fetches:
        fetch.start()

    def body(gate, gate_change, up, up_change):
        step = pl.program_id(0)
        for pair in range(IN_STEP // 2):
            for at, (master, second) in enumerate(((gate, gate_change), (up, up_change))):
                two = slice(2 * pair, 2 * pair + 2)
                merged = master[two] + second[two].astype(jnp.float32)
                turned = merged.reshape(2 * rows, width).T.astype(jnp.bfloat16)
                first = pl.multiple_of(step * (IN_STEP * part), 2 * part) + (2 * pair + at) * part
                for peer in range(peers):
                    send[peer, pl.ds(first, part), :] = turned[peer * part : (peer + 1) * part]

    block = pl.BlockSpec((IN_STEP, rows, width), lambda i: (i, 0, 0), pipeline_mode=pl.Buffered(8))
    pltpu.emit_pipeline(body, grid=(experts // IN_STEP,), in_specs=[block] * 4)(master_gate, second_gate, master_up, second_up)
    for fetch in fetches:
        fetch.wait()
    router = (weight[...] * gain[...]).astype(jnp.bfloat16)
    half = router.shape[0] // 2
    router = jnp.concatenate([router[:half], router[half:]], axis=1)
    for peer in range(peers):
        send[peer, experts * part :, :] = router


def pack(master_gate, second_gate, master_up, second_up, weight, gain, peers):
    experts, rows, width = master_gate.shape
    part = width // peers
    lines = experts * part + weight.shape[0] // 2
    big = [pltpu.with_memory_space_constraint(x, pltpu.HBM) for x in (master_gate, second_gate, master_up, second_up, weight, gain)]
    in_hbm = pl.BlockSpec(memory_space=pltpu.HBM)
    in_vmem = pl.BlockSpec(memory_space=pltpu.VMEM)
    return pl.pallas_call(
        functools.partial(pack_kernel, part),
        in_specs=[in_hbm] * 6,
        out_specs=in_vmem,
        out_shape=pltpu.VMEM((peers, lines, 2 * rows), jnp.bfloat16),
        scratch_shapes=[
            pltpu.VMEM(weight.shape, jnp.float32),
            pltpu.VMEM(gain.shape, jnp.float32),
            pltpu.SemaphoreType.DMA((2,)),
        ],
        compiler_params=pltpu.CompilerParams(vmem_limit_bytes=32 * MIB),
        cost_estimate=pl.CostEstimate(flops=2 * master_gate.size, bytes_accessed=12 * master_gate.size, transcendentals=0),
        name="pack",
    )(*big)


def unpack_kernel(part, taken, final_gate, final_up, ready_gate, ready_up, sent):
    peers, _, lanes = taken.shape
    experts = final_gate.shape[0]
    steps = experts // OUT_STEP

    def out(step, at):
        ready, final = ((ready_gate, final_gate), (ready_up, final_up))[at]
        some = pl.ds(step * OUT_STEP, OUT_STEP)
        return pltpu.make_async_copy(ready.at[some], final.at[some], sent.at[at, step])

    @pl.loop(0, steps)
    def _(step):
        for at, ready in enumerate((ready_gate, ready_up)):
            for pair in range(OUT_STEP // 2):
                first = pl.multiple_of(step * (OUT_STEP * part), 2 * part) + (2 * pair + at) * part
                expert = step * OUT_STEP + 2 * pair
                for couple in range(peers // 2):
                    columns = slice(couple * lanes, (couple + 1) * lanes)
                    ready[expert, :, columns], ready[expert + 1, :, columns] = joined(
                        taken[2 * couple, pl.ds(first, part), :], taken[2 * couple + 1, pl.ds(first, part), :]
                    )
            out(step, at).start()

    @pl.loop(0, steps)
    def _(step):
        out(step, 0).wait()
        out(step, 1).wait()


def unpack(taken, experts, rows, part):
    peers = taken.shape[0]
    shape = (experts, part, peers * rows)
    out = jax.ShapeDtypeStruct(shape, jnp.bfloat16)
    return pl.pallas_call(
        functools.partial(unpack_kernel, part),
        in_specs=[pl.BlockSpec(memory_space=pltpu.VMEM)],
        out_specs=[pl.BlockSpec(memory_space=pltpu.HBM)] * 2,
        out_shape=[out, out],
        scratch_shapes=[
            pltpu.VMEM(shape, jnp.bfloat16),
            pltpu.VMEM(shape, jnp.bfloat16),
            pltpu.SemaphoreType.DMA((2, experts // OUT_STEP)),
        ],
        compiler_params=pltpu.CompilerParams(vmem_limit_bytes=32 * MIB),
        cost_estimate=pl.CostEstimate(flops=taken.size * 64, bytes_accessed=4 * taken.size, transcendentals=0),
        name="unpack",
    )(pltpu.with_memory_space_constraint(taken, pltpu.VMEM))


def router_kernel(*refs):
    *pieces, out, turned = refs
    me = lax.axis_index("expert")
    for other, piece in enumerate(pieces):
        peers, half, lanes = piece.shape
        first = pl.multiple_of((me ^ other) * (2 * half), 2 * half)
        for couple in range(peers // 2):
            columns = slice(couple * lanes, (couple + 1) * lanes)
            turned[pl.ds(first, half), columns], turned[pl.ds(first + half, half), columns] = joined(
                piece[2 * couple], piece[2 * couple + 1]
            )
    out[...] = turned[...].T


def spread_router(own):
    columns = lax.axis_size("expert")
    pieces = [own]
    for other in range(1, columns):
        pieces.append(lax.ppermute(own, "expert", [(i, i ^ other) for i in range(columns)]))
    peers, half, lanes = own.shape
    rows = peers * lanes // 2
    return pl.pallas_call(
        router_kernel,
        in_specs=[pl.BlockSpec(memory_space=pltpu.VMEM)] * columns,
        out_specs=pl.BlockSpec(memory_space=pltpu.VMEM),
        out_shape=jax.ShapeDtypeStruct((rows, columns * 2 * half), jnp.bfloat16),
        scratch_shapes=[pltpu.VMEM((columns * 2 * half, rows), jnp.bfloat16)],
        compiler_params=pltpu.CompilerParams(vmem_limit_bytes=16 * MIB),
        name="router",
    )(*pieces)


def per_device(master_gate, second_gate, master_up, second_up, router_weight, router_gain):
    experts, rows, width = master_gate.shape
    peers = lax.axis_size("shard")
    part = width // peers
    send = pack(master_gate, second_gate, master_up, second_up, router_weight.T, router_gain[None], peers)
    taken = lax.all_to_all(send, "shard", 0, 0, tiled=True)
    serve_router = spread_router(taken[:, experts * part :])
    final_gate, final_up = unpack(taken, experts, rows, part)
    return (final_gate, final_up, serve_router)


def solution(mesh):
    placed = (
        P("expert", "shard", None),
        P("expert", "shard", None),
        P("expert", "shard", None),
        P("expert", "shard", None),
        P("shard", "expert"),
        P("shard"),
    )
    return jax.shard_map(
        per_device,
        mesh=mesh,
        in_specs=placed,
        out_specs=(P("expert", "shard", None), P("expert", "shard", None), P()),
        check_vma=False,
    )
```
